512 devices in a mesh: seq: 32 (over x, y), batch: 16 (over z, core).
Axes of the slice: x: 4, y: 8, z: 8, core: 2. Of those that a mesh axis runs over, the one named last changes fastest.
Arguments:
- queries: bfloat16 [64, 4096], P('batch', 'seq'), may hold values from -210 to 210
- key_cache: bfloat16 [64, 4096, 2048], P('batch', 'seq'), may hold values from -6 to 6
- value_cache: bfloat16 [64, 4096, 2048], P('batch', 'seq'), may hold values from -12 to 12
- new_key: bfloat16 [64, 2048], P('batch'), may hold values from -6 to 6
- new_value: bfloat16 [64, 2048], P('batch'), may hold values from -12 to 12
- page_table: int32 [64, 32], P('batch', 'seq'), may hold values from 0 to 3, as said below
- counts: int32 [64, 32], P('batch', 'seq'), may hold values from 1 to 128
- offsets: int32 [64], P('batch'), may hold values from 0 to 3968
- w_out: bfloat16 [4096, 4608], P('seq', 'batch'), may hold values from -0.09375 to 0.09375
Outputs:
- projected: bfloat16 [64, 4608], P('seq', 'batch')
The draws below stay inside these ranges and needn't reach their ends.
Inputs may be any that keep to these rules, and one draw needn't show every extreme that they name: `page_table`: for each group of 4 requests and each index along seq, the slots of that index's 1 pages of the group's requests are all different.
All inputs are finite; a program needn't handle non-finite values.
Results may differ from the reference program's by a relative error of at most 0.005.
Values may be sent and summed in bfloat16 or wider, within the bound.
No kernel may reach another device: no remote copies, remote signals or barrier semaphores. Data moves between devices by JAX's collectives and lax.ppermute only.
A program may use at most 64 MiB of HBM per device.

```python
import jax
import jax.numpy as jnp
from jax import lax

D = 4608
HEADS = 32
KVH = 16
HD = 128
QSCALAR = 144
PAGE = 128
REQ_DEV = 4
PAGES_DEV = 1
BATCH = 64
SLOTS = 4
NPAGES = 32
N_SEQ = 32
N_BATCH = 16


def slot_table(key):
    subkeys = jax.random.split(jax.random.fold_in(key, 11), N_BATCH * N_SEQ)
    orders = jax.vmap(lambda subkey: jax.random.permutation(subkey, SLOTS))(subkeys)
    orders = orders.reshape(N_BATCH, N_SEQ, REQ_DEV, PAGES_DEV).transpose(0, 2, 1, 3)
    return orders.reshape(N_BATCH * REQ_DEV, N_SEQ * PAGES_DEV).astype(jnp.int32)


def draw_page_table(key, part):
    return slot_table(key)


def draw_queries(key, part):
    drawn = 3.0 * jnp.clip(jax.random.normal(jax.random.fold_in(key, 31), (BATCH, HEADS, HD), jnp.float32), -6.0, 6.0)
    return drawn.reshape(BATCH, HEADS * HD).astype(jnp.bfloat16)


def draw_key_cache(key, part):
    key_values = jnp.clip(jax.random.normal(jax.random.fold_in(key, 41), (N_BATCH * SLOTS, N_SEQ * PAGE, KVH * HD), jnp.float32), -6.0, 6.0)
    return key_values.astype(jnp.bfloat16)


def draw_new_key(key, part):
    fresh_keys = jnp.clip(jax.random.normal(jax.random.fold_in(key, 53), (BATCH, KVH * HD), jnp.float32), -6.0, 6.0)
    return fresh_keys.astype(jnp.bfloat16)


def place_ends(result, key, low, top_value):
    place = [jax.random.randint(jax.random.fold_in(key, axis), (), 0, length) for axis, length in enumerate(result.shape)]
    longest = result.shape.index(max(result.shape))
    beside = place[:longest] + [(place[longest] + 1) % result.shape[longest]] + place[longest + 1:]
    return result.at[tuple(place)].set(low).at[tuple(beside)].set(top_value)


def shard_levels(rng, dims, cuts, smallest, top_value):
    level = 1.0
    for axis_at, parts in cuts:
        draws = jax.random.uniform(jax.random.fold_in(jax.random.fold_in(rng, 6), axis_at), (parts,), jnp.float32, smallest / len(cuts), top_value / len(cuts))
        level = level * jnp.repeat(jnp.exp(draws), dims[axis_at] // parts).reshape((-1,) + (1,) * (len(dims) - 1 - axis_at))
    return level


def noise(key, shape, deviation, most, pieces=(), kind=jnp.bfloat16):
    values = deviation * jax.random.normal(key, shape, jnp.float32)
    if pieces:
        values = values * shard_levels(key, shape, pieces, -0.22, 0.18)
    return jnp.clip(values, -most, most).astype(kind)


def setup_inputs(seed: int = 0) -> dict:
    arg_keys = jax.random.split(jax.random.key(seed), 10)
    queries = draw_queries(jax.random.fold_in(arg_keys[9], 71), 0)
    key_cache = draw_key_cache(jax.random.fold_in(arg_keys[9], 71), 0)
    value_cache = noise(arg_keys[2], (SLOTS * N_BATCH, PAGE * N_SEQ, KVH * HD), 2.0, 12.0, ((0, 16), (1, 32)))
    new_key = draw_new_key(jax.random.fold_in(arg_keys[9], 71), 0)
    new_value = noise(arg_keys[4], (BATCH, KVH * HD), 2.0, 12.0, ((0, 16),))
    page_table = draw_page_table(jax.random.fold_in(arg_keys[9], 71), 0)
    counts = place_ends(jax.random.randint(arg_keys[6], (BATCH, NPAGES), 1, PAGE + 1), jax.random.fold_in(arg_keys[6], 1), 1, PAGE).astype(jnp.int32)
    offsets = place_ends(jax.random.randint(arg_keys[7], (BATCH,), 0, NPAGES * PAGE - PAGE + 1), jax.random.fold_in(arg_keys[7], 1), 0, NPAGES * PAGE - PAGE).astype(jnp.int32)
    w_out = noise(arg_keys[8], (HEADS * HD, D), (HEADS * HD) ** -0.5, 0.09375, ((0, 32), (1, 16)))
    return dict(queries=queries, key_cache=key_cache, value_cache=value_cache, new_key=new_key, new_value=new_value, page_table=page_table, counts=counts, offsets=offsets, w_out=w_out)


floor_score = -1.0e30


def reference(queries, key_cache, value_cache, new_key, new_value, page_table, counts, offsets, w_out):
    groups = HEADS // KVH
    score_multiplier = QSCALAR ** -0.5
    query_lattice = queries.astype(jnp.float32).reshape(BATCH, KVH, groups, HD)
    owner_row = (jnp.arange(BATCH, dtype=jnp.int32) // REQ_DEV) * SLOTS
    token_index = jnp.arange(PAGE, dtype=jnp.int32)

    def page_block(column_tile_block):
        key_slab = lax.dynamic_slice_in_dim(key_cache, column_tile_block * PAGE, PAGE, 1)
        value_slab = lax.dynamic_slice_in_dim(value_cache, column_tile_block * PAGE, PAGE, 1)
        slot_cols = lax.dynamic_slice_in_dim(page_table, column_tile_block * PAGES_DEV, PAGES_DEV, 1)
        live_counts = lax.dynamic_slice_in_dim(counts, column_tile_block * PAGES_DEV, PAGES_DEV, 1)
        slot_rows = owner_row[:, None] + slot_cols
        key_rows = key_slab[slot_rows].astype(jnp.float32).reshape(BATCH, PAGES_DEV * PAGE, KVH, HD)
        value_rows = value_slab[slot_rows].astype(jnp.float32).reshape(BATCH, PAGES_DEV * PAGE, KVH, HD)
        page_start = (column_tile_block * PAGES_DEV + jnp.arange(PAGES_DEV, dtype=jnp.int32)) * PAGE
        live_mask = (token_index[None, None, :] < live_counts[:, :, None]) & (
            page_start[None, :, None] + token_index[None, None, :] >= offsets[:, None, None])
        live_mask = live_mask.reshape(BATCH, PAGES_DEV * PAGE)[:, None, None, :]
        scores = jnp.einsum("bkgd,btkd->bkgt", query_lattice, key_rows) * score_multiplier
        peak_score = jnp.max(jnp.where(live_mask, scores, floor_score), axis=-1)
        weights = jnp.where(live_mask, jnp.exp(scores - peak_score[..., None]), 0.0)
        block_total = jnp.sum(weights, axis=-1)
        rounded = lax.optimization_barrier(weights.astype(jnp.bfloat16)).astype(jnp.float32)
        block_sum = jnp.einsum("bkgt,btkd->bkgd", rounded, value_rows)
        return peak_score, block_total, block_sum

    peaks, totals, sums = lax.map(page_block, jnp.arange(N_SEQ, dtype=jnp.int32))
    incoming_keys = new_key.astype(jnp.float32).reshape(BATCH, KVH, HD)
    incoming_score = jnp.einsum("pcoz,pcz->pco", query_lattice, incoming_keys) * score_multiplier
    top_score = jnp.maximum(jnp.max(peaks, axis=0), incoming_score)
    factor = jnp.exp(peaks - top_score[None])
    own_weight = jnp.exp(incoming_score - top_score)
    denominator = jnp.sum(totals * factor, axis=0) + own_weight
    fresh_value = new_value.astype(jnp.float32).reshape(BATCH, KVH, 1, HD)
    numerator = jnp.sum(sums * factor[..., None], axis=0) + own_weight[..., None] * fresh_value
    attention = (numerator / denominator[..., None]).astype(jnp.bfloat16).reshape(BATCH, HEADS * HD)
    return jnp.dot(attention, w_out, preferred_element_type=jnp.float32).astype(jnp.bfloat16)
```

```python
import jax
import jax.numpy as jnp
from jax import lax
from jax.experimental import pallas as pl
from jax.experimental.pallas import tpu as pltpu
from jax.sharding import Mesh
from jax.sharding import PartitionSpec as P

HEADS = 32
KVH = 16
HD = 128
QSCALAR = 144
SEQ = ("seq_0", "seq_1")
FLOOR = -1e30
CHUNKS = 4


def by_request(row, values):
    request = row & 3
    picked = jnp.where(request == 0, values[0], values[1])
    return jnp.where(request >= 2, jnp.where(request == 2, values[2], values[3]), picked)


def attend_pages(meta, q_ref, k_far, v_far, out_ref, k_ref, v_ref, arrived):
    row = lax.broadcasted_iota(jnp.int32, (8, HD), 0)
    lane = lax.broadcasted_iota(jnp.int32, (8, HD), 1)
    request = row & 3
    slots = [meta[r] for r in range(4)]
    live = (lane < by_request(row, [meta[4 + r] for r in range(4)])) & (
        lane >= by_request(row, [meta[8 + r] for r in range(4)])
    )
    width = KVH * HD // CHUNKS
    loads = []
    for i, (far, near) in enumerate(((k_far, k_ref), (v_far, v_ref))):
        for c in range(CHUNKS):
            part = (slice(None), slice(None), pl.ds(c * width, width))
            loads.append(
                pltpu.make_async_copy(far.at[part], near.at[part], arrived.at[i * CHUNKS + c])
            )
    for load in loads:
        load.start()
    queries = q_ref[...].astype(jnp.float32)

    def apart(x):
        return jnp.concatenate(
            [jnp.where(request == r, x, 0.0) for r in range(4)], axis=1
        ).astype(jnp.bfloat16)

    spread, stats = [], []
    for k in range(KVH):
        if k % (KVH // CHUNKS) == 0:
            loads[k // (KVH // CHUNKS)].wait()
        keys = jnp.concatenate([k_ref[slots[r], :, k * HD : (k + 1) * HD] for r in range(4)], axis=1)
        scores = lax.dot_general(
            apart(queries[8 * k : 8 * k + 8]),
            keys,
            (((1,), (1,)), ((), ())),
            preferred_element_type=jnp.float32,
        ) * (QSCALAR ** (-0.5))
        peak = jnp.max(jnp.where(live, scores, FLOOR), axis=1, keepdims=True)
        mark = peak.astype(jnp.bfloat16).astype(jnp.float32)
        weights = jnp.where(live, jnp.exp(scores - mark), 0.0)
        total = jnp.sum(weights, axis=1, keepdims=True)
        coarse = total.astype(jnp.bfloat16).astype(jnp.float32)
        spread.append(apart(weights))
        stats.append(jnp.where(lane == 0, mark, jnp.where(lane == 1, coarse, total - coarse)))
    for k in range(KVH):
        if k % (KVH // CHUNKS) == 0:
            loads[CHUNKS + k // (KVH // CHUNKS)].wait()
        values = jnp.concatenate(
            [v_ref[slots[r], :, k * HD : (k + 1) * HD] for r in range(4)], axis=0
        )
        sums = jnp.dot(spread[k], values, preferred_element_type=jnp.float32)
        even = jnp.where(row < 4, sums, pltpu.roll(stats[k], 4, 0))
        odd = jnp.where(row < 4, pltpu.roll(sums, 4, 0), stats[k])
        out_ref[2 * k] = even.astype(jnp.bfloat16)
        out_ref[2 * k + 1] = odd.astype(jnp.bfloat16)


def merge_blocks(blocks_ref, new_score_ref, new_value_ref, out_ref):
    blocks = blocks_ref[...].astype(jnp.float32)
    sums = blocks[:, 0:4, :]
    mark = blocks[:, 4:8, 0:1]
    total = blocks[:, 4:8, 1:2] + blocks[:, 4:8, 2:3]
    new_score = new_score_ref[...]
    top = jnp.maximum(jnp.max(mark, axis=0), new_score)
    factor = jnp.exp(mark - top[None])
    own = jnp.exp(new_score - top)
    denominator = jnp.sum(total * factor, axis=0) + own
    numerator = jnp.sum(sums * factor, axis=0) + own * new_value_ref[...]
    attention = (numerator / denominator).astype(jnp.bfloat16)
    out_ref[...] = jnp.broadcast_to(attention[None], out_ref.shape)


def on_device(
    queries, key_cache, value_cache, new_key, new_value, page_table, counts, offsets, w_out
):
    requests = queries.shape[0]
    place = lax.axis_index(SEQ)
    peers = lax.axis_size(SEQ)
    groups = lax.axis_size("batch")
    page_len = key_cache.shape[1]
    vmem = pl.BlockSpec(memory_space=pltpu.VMEM)
    smem = pl.BlockSpec(memory_space=pltpu.SMEM)
    hbm = pl.BlockSpec(memory_space=pltpu.HBM)

    def near(x):
        return pltpu.with_memory_space_constraint(x, pltpu.VMEM)

    def far(x):
        return pltpu.with_memory_space_constraint(x, pltpu.HBM)

    all_queries = lax.all_to_all(
        jnp.broadcast_to(queries[None], (peers, *queries.shape)), SEQ, 0, 0, tiled=True
    )
    meta = jnp.concatenate([page_table[:, 0], counts[:, 0], offsets - place * page_len])
    column = (place // (HEADS // KVH)) * HD
    own_key = lax.dynamic_slice_in_dim(new_key, column, HD, 1).astype(jnp.float32)
    own_value = lax.dynamic_slice_in_dim(new_value, column, HD, 1).astype(jnp.float32)
    new_score = jnp.sum(queries.astype(jnp.float32) * own_key, axis=1, keepdims=True) * (
        QSCALAR ** (-0.5)
    )

    blocks = pl.pallas_call(
        attend_pages,
        out_shape=pltpu.VMEM((HEADS, 8, HD), jnp.bfloat16),
        in_specs=[smem, vmem, hbm, hbm],
        out_specs=vmem,
        scratch_shapes=[
            pltpu.VMEM(key_cache.shape, key_cache.dtype),
            pltpu.VMEM(value_cache.shape, value_cache.dtype),
            pltpu.SemaphoreType.DMA((2 * CHUNKS,)),
        ],
        compiler_params=pltpu.CompilerParams(vmem_limit_bytes=16 << 20),
    )(meta, near(all_queries.reshape(HEADS * requests, HD)), far(key_cache), far(value_cache))
    blocks = lax.all_to_all(blocks, SEQ, 0, 0, tiled=True)
    attention = pl.pallas_call(
        merge_blocks,
        out_shape=pltpu.VMEM((groups, requests, HD), jnp.bfloat16),
        in_specs=[vmem, vmem, vmem],
        out_specs=vmem,
        compiler_params=pltpu.CompilerParams(vmem_limit_bytes=16 << 20),
    )(near(blocks), near(new_score), near(own_value))
    attention = lax.all_to_all(attention, "batch", 0, 0, tiled=True)
    partial = jnp.dot(
        attention.reshape(groups * requests, HD), w_out, preferred_element_type=jnp.float32
    )
    partial = partial.reshape(peers, -1, partial.shape[1])
    partial = lax.all_to_all(partial, SEQ, 0, 0, tiled=True)
    return jnp.sum(partial, axis=0).astype(jnp.bfloat16)


def solution(mesh):
    torus = Mesh(mesh.devices.reshape(4, 8, mesh.shape["batch"]), ("seq_0", "seq_1", "batch"))
    in_specs = (
        P("batch", SEQ),
        P("batch", SEQ, None),
        P("batch", SEQ, None),
        P("batch", None),
        P("batch", None),
        P("batch", SEQ),
        P("batch", SEQ),
        P("batch"),
        P(SEQ, "batch"),
    )
    return jax.shard_map(
        on_device, mesh=torus, in_specs=in_specs, out_specs=P(SEQ, "batch"), check_vma=False
    )
```

```python
import jax
import jax.numpy as jnp
from jax import lax
from jax.experimental import pallas as pl
from jax.experimental.pallas import tpu as pltpu
from jax.sharding import Mesh
from jax.sharding import PartitionSpec as P

HEADS = 32
KVH = 16
HD = 128
QSCALAR = 144
SCALE = QSCALAR ** (-0.5)
SEQ = ("seq_0", "seq_1")
FLOOR = -1e30
LOADS = 12


def by_request(row, values):
    request = row & 3
    picked = jnp.where(request == 0, values[0], values[1])
    return jnp.where(request >= 2, jnp.where(request == 2, values[2], values[3]), picked)


def fetch_pages(
    place_ref, table_ref, counts_ref, offsets_ref, q_ref, new_key_ref, new_value_ref,
    k_far, v_far, k_ref, v_ref, later_ref, limits_ref, own_ref, arrived,
):
    half = v_ref.shape[2]
    loads = []
    for r in range(4):
        slot = table_ref[r]
        for source, target in (
            (k_far.at[slot], k_ref.at[r]),
            (v_far.at[slot, :, pl.ds(0, half)], v_ref.at[r]),
            (v_far.at[slot, :, pl.ds(half, half)], later_ref.at[r]),
        ):
            loads.append(pltpu.make_async_copy(source, target, arrived.at[len(loads)]))
    for load in loads:
        load.start()
    place = place_ref[0]
    row = lax.broadcasted_iota(jnp.int32, (8, HD), 0)
    limits_ref[0:8] = by_request(row, [counts_ref[r] for r in range(4)])
    limits_ref[8:16] = by_request(row, [offsets_ref[r] - place * HD for r in range(4)])
    column = pl.multiple_of((place // (HEADS // KVH)) * HD, HD)
    key = new_key_ref[:, pl.ds(column, HD)].astype(jnp.float32)
    score = jnp.sum(q_ref[...].astype(jnp.float32) * key, axis=1, keepdims=True) * SCALE
    own_ref[0:4] = jnp.broadcast_to(score, (4, HD))
    own_ref[4:8] = new_value_ref[:, pl.ds(column, HD)].astype(jnp.float32)
    for load in loads:
        load.wait()


def attend_pages(q_ref, k_ref, v_ref, later_far, limits_ref, out_ref, later_ref, arrived):
    later = pltpu.make_async_copy(later_far, later_ref, arrived)
    later.start()
    row = lax.broadcasted_iota(jnp.int32, (8, HD), 0)
    lane = lax.broadcasted_iota(jnp.int32, (8, HD), 1)
    request = row & 3
    live = (lane < limits_ref[0:8]) & (lane >= limits_ref[8:16])
    queries = q_ref[...].astype(jnp.float32)

    def apart(x):
        return jnp.concatenate(
            [jnp.where(request == r, x, 0.0) for r in range(4)], axis=1
        ).astype(jnp.bfloat16)

    for k in range(KVH):
        cols = slice(k * HD, (k + 1) * HD)
        keys = jnp.concatenate([k_ref[r, :, cols] for r in range(4)], axis=1)
        scores = lax.dot_general(
            apart(queries[8 * k : 8 * k + 8]),
            keys,
            (((1,), (1,)), ((), ())),
            preferred_element_type=jnp.float32,
        ) * SCALE
        peak = jnp.max(jnp.where(live, scores, FLOOR), axis=1, keepdims=True)
        weights = jnp.where(live, jnp.exp(scores - peak), 0.0)
        if k == KVH // 2:
            later.wait()
        held = v_ref if k < KVH // 2 else later_ref
        cols = slice(k % (KVH // 2) * HD, (k % (KVH // 2) + 1) * HD)
        values = jnp.concatenate([held[r, :, cols] for r in range(4)], axis=0)
        sums = jnp.dot(apart(weights), values, preferred_element_type=jnp.float32)
        mark = peak.astype(jnp.bfloat16).astype(jnp.float32)
        shift = jnp.exp(jnp.minimum(peak - mark, 64.0))
        total = jnp.sum(weights, axis=1, keepdims=True) * shift
        coarse = total.astype(jnp.bfloat16).astype(jnp.float32)
        sums = sums * shift
        stats = jnp.where(lane == 0, mark, jnp.where(lane == 1, coarse, total - coarse))
        even = jnp.where(row < 4, sums, pltpu.roll(stats, 4, 0))
        odd = jnp.where(row < 4, pltpu.roll(sums, 4, 0), stats)
        out_ref[2 * k] = even.astype(jnp.bfloat16)
        out_ref[2 * k + 1] = odd.astype(jnp.bfloat16)


def merge_blocks(blocks_ref, own_ref, out_ref):
    blocks = blocks_ref[...].astype(jnp.float32)
    sums = blocks[:, 0:4, :]
    mark = blocks[:, 4:8, 0:1]
    total = blocks[:, 4:8, 1:2] + blocks[:, 4:8, 2:3]
    new_score = own_ref[0:4, 0:1]
    top = jnp.maximum(jnp.max(mark, axis=0), new_score)
    factor = jnp.exp(mark - top[None])
    own = jnp.exp(new_score - top)
    denominator = jnp.sum(total * factor, axis=0) + own
    numerator = jnp.sum(sums * factor, axis=0) + own * own_ref[4:8]
    attention = (numerator / denominator).astype(jnp.bfloat16)
    out_ref[...] = jnp.broadcast_to(attention[None], out_ref.shape)


def on_device(
    queries, key_cache, value_cache, new_key, new_value, page_table, counts, offsets, w_out
):
    requests = queries.shape[0]
    place = lax.axis_index(SEQ)
    peers = lax.axis_size(SEQ)
    groups = lax.axis_size("batch")
    vmem = pl.BlockSpec(memory_space=pltpu.VMEM)
    smem = pl.BlockSpec(memory_space=pltpu.SMEM)
    hbm = pl.BlockSpec(memory_space=pltpu.HBM)
    half = (*value_cache.shape[:2], value_cache.shape[2] // 2)
    small = pltpu.CompilerParams(vmem_limit_bytes=8 << 20)

    def near(x):
        return pltpu.with_memory_space_constraint(x, pltpu.VMEM)

    def far(x):
        return pltpu.with_memory_space_constraint(x, pltpu.HBM)

    all_queries = lax.all_to_all(
        jnp.broadcast_to(queries[None], (peers, *queries.shape)), SEQ, 0, 0, tiled=True
    )
    keys, values, later, limits, own = pl.pallas_call(
        fetch_pages,
        out_shape=(
            pltpu.VMEM(key_cache.shape, key_cache.dtype),
            pltpu.VMEM(half, value_cache.dtype),
            pltpu.HBM(half, value_cache.dtype),
            pltpu.VMEM((16, HD), jnp.int32),
            pltpu.VMEM((8, HD), jnp.float32),
        ),
        in_specs=[smem] * 4 + [vmem] * 3 + [hbm] * 2,
        out_specs=(vmem, vmem, hbm, vmem, vmem),
        scratch_shapes=[pltpu.SemaphoreType.DMA((LOADS,))],
        compiler_params=small,
    )(
        place.reshape(1), page_table[:, 0], counts[:, 0], offsets,
        queries, new_key, new_value, far(key_cache), far(value_cache),
    )
    blocks = pl.pallas_call(
        attend_pages,
        out_shape=pltpu.VMEM((HEADS, 8, HD), jnp.bfloat16),
        in_specs=[vmem, vmem, vmem, hbm, vmem],
        out_specs=vmem,
        scratch_shapes=[pltpu.VMEM(half, value_cache.dtype), pltpu.SemaphoreType.DMA],
        compiler_params=small,
    )(near(all_queries.reshape(HEADS * requests, HD)), near(keys), near(values), far(later), near(limits))
    blocks = lax.all_to_all(blocks, SEQ, 0, 0, tiled=True)
    attention = pl.pallas_call(
        merge_blocks,
        out_shape=pltpu.VMEM((groups, requests, HD), jnp.bfloat16),
        in_specs=[vmem] * 2,
        out_specs=vmem,
        compiler_params=small,
    )(near(blocks), near(own))
    attention = lax.all_to_all(attention, "batch", 0, 0, tiled=True)
    partial = jnp.dot(
        attention.reshape(groups * requests, HD), w_out, preferred_element_type=jnp.float32
    )
    partial = partial.reshape(peers, -1, partial.shape[1])
    partial = lax.all_to_all(partial, SEQ, 0, 0, tiled=True)
    return jnp.sum(partial, axis=0).astype(jnp.bfloat16)


def solution(mesh):
    torus = Mesh(mesh.devices.reshape(4, 8, mesh.shape["batch"]), ("seq_0", "seq_1", "batch"))
    in_specs = (
        P("batch", SEQ),
        P("batch", SEQ, None),
        P("batch", SEQ, None),
        P("batch", None),
        P("batch", None),
        P("batch", SEQ),
        P("batch", SEQ),
        P("batch"),
        P(SEQ, "batch"),
    )
    return jax.shard_map(
        on_device, mesh=torus, in_specs=in_specs, out_specs=P(SEQ, "batch"), check_vma=False
    )
```

```python
import jax
import jax.numpy as jnp
from jax import lax
from jax.experimental import pallas as pl
from jax.experimental.pallas import tpu as pltpu
from jax.sharding import Mesh
from jax.sharding import PartitionSpec as P

HEADS = 32
KVH = 16
HD = 128
QSCALAR = 144
SCALE = QSCALAR ** (-0.5)
SEQ = ("seq_0", "seq_1")
FLOOR = -1e30
UNROLL = 4


def by_request(row, values):
    request = row & 3
    picked = jnp.where(request == 0, values[0], values[1])
    return jnp.where(request >= 2, jnp.where(request == 2, values[2], values[3]), picked)


def fetch_pages(
    table_far, counts_far, offsets_far, q_far, new_key_far, new_value_far, k_far, v_far,
    k_ref, v_ref, rows_ref, own_ref,
    table_ref, counts_ref, offsets_ref, q_ref, new_key_ref, new_value_ref, arrived,
):
    place = lax.axis_index(SEQ)
    column = pl.multiple_of((place // (HEADS // KVH)) * HD, HD)
    half = v_ref.shape[2]
    loads = [
        pltpu.make_async_copy(source, target, arrived.at[i])
        for i, (source, target) in enumerate(
            (
                (table_far, table_ref),
                (counts_far, counts_ref),
                (offsets_far, offsets_ref),
                (q_far, q_ref),
                (new_key_far.at[:, pl.ds(column, HD)], new_key_ref),
                (new_value_far.at[:, pl.ds(column, HD)], new_value_ref),
                (k_far, k_ref),
                (v_far.at[:, :, pl.ds(0, half)], v_ref),
            )
        )
    ]
    for load in loads:
        load.start()
    row = lax.broadcasted_iota(jnp.int32, (8, HD), 0)
    for load in loads[:6]:
        load.wait()
    rows_ref[0] = by_request(row, [table_ref[r] for r in range(4)])
    rows_ref[1] = by_request(row, [counts_ref[r] for r in range(4)])
    rows_ref[2] = by_request(row, [offsets_ref[r] - place * HD for r in range(4)])
    key = new_key_ref[...].astype(jnp.float32)
    score = jnp.sum(q_ref[...].astype(jnp.float32) * key, axis=1, keepdims=True) * SCALE
    own_ref[0:4] = jnp.broadcast_to(score, (4, HD))
    own_ref[4:8] = new_value_ref[...].astype(jnp.float32)
    for load in loads[6:]:
        load.wait()


def attend_pages(
    q_ref, k_ref, v_ref, v_far, rows_ref, out_ref,
    later_ref, wide_ref, scores_ref, stats_ref, arrived,
):
    half = later_ref.shape[2]
    later = pltpu.make_async_copy(v_far.at[:, :, pl.ds(half, half)], later_ref, arrived)
    later.start()
    row = lax.broadcasted_iota(jnp.int32, (8, HD), 0)
    lane = lax.broadcasted_iota(jnp.int32, (8, HD), 1)
    slot = rows_ref[0]

    def apart(x):
        return jnp.concatenate(
            [jnp.where(slot == i, x, 0.0) for i in range(4)], axis=1
        ).astype(jnp.bfloat16)

    wide_ref[...] = q_ref[...].astype(jnp.float32)

    def score(i, carry):
        for j in range(UNROLL):
            k = i * UNROLL + j
            rows = pl.ds(pl.multiple_of(k * 8, 8), 8)
            cols = pl.ds(pl.multiple_of(k * HD, HD), HD)
            keys = jnp.concatenate([k_ref[i, :, cols] for i in range(4)], axis=1)
            scores_ref[rows] = lax.dot_general(
                apart(wide_ref[rows]),
                keys,
                (((1,), (1,)), ((), ())),
                preferred_element_type=jnp.float32,
            )
        return carry

    lax.fori_loop(0, KVH // UNROLL, score, 0)
    live = ((lane < rows_ref[1]) & (lane >= rows_ref[2]))[None]
    scores = scores_ref[...].reshape(KVH, 8, HD) * SCALE
    peak = jnp.max(jnp.where(live, scores, FLOOR), axis=2, keepdims=True)
    weights = jnp.where(live, jnp.exp(scores - peak), 0.0)
    mark = peak.astype(jnp.bfloat16).astype(jnp.float32)
    shift = jnp.exp(jnp.minimum(peak - mark, 64.0))
    total = jnp.sum(weights, axis=2, keepdims=True) * shift
    coarse = total.astype(jnp.bfloat16).astype(jnp.float32)
    stats = jnp.where(lane == 1, coarse, jnp.where(lane == 2, total - coarse, shift))
    scores_ref[...] = weights.reshape(KVH * 8, HD)
    stats_ref[...] = jnp.where(lane == 0, mark, stats).reshape(KVH * 8, HD)

    def value(held, base):
        def step(i, carry):
            for j in range(UNROLL):
                k = i * UNROLL + j
                rows = pl.ds(pl.multiple_of((base + k) * 8, 8), 8)
                cols = pl.ds(pl.multiple_of(k * HD, HD), HD)
                values = jnp.concatenate([held[i, :, cols] for i in range(4)], axis=0)
                sums = jnp.dot(
                    apart(scores_ref[rows]), values, preferred_element_type=jnp.float32
                )
                stats = stats_ref[rows]
                sums = sums * stats[:, 3:4]
                even = jnp.where(row < 4, sums, pltpu.roll(stats, 4, 0))
                odd = jnp.where(row < 4, pltpu.roll(sums, 4, 0), stats)
                out_ref[2 * (base + k)] = even.astype(jnp.bfloat16)
                out_ref[2 * (base + k) + 1] = odd.astype(jnp.bfloat16)
            return carry

        return step

    lax.fori_loop(0, KVH // 2 // UNROLL, value(v_ref, 0), 0)
    later.wait()
    lax.fori_loop(0, KVH // 2 // UNROLL, value(later_ref, KVH // 2), 0)


def merge_blocks(blocks_ref, own_ref, out_ref):
    blocks = blocks_ref[...].astype(jnp.float32)
    sums = blocks[:, 0:4, :]
    mark = blocks[:, 4:8, 0:1]
    total = blocks[:, 4:8, 1:2] + blocks[:, 4:8, 2:3]
    new_score = own_ref[0:4, 0:1]
    top = jnp.maximum(jnp.max(mark, axis=0), new_score)
    factor = jnp.exp(mark - top[None])
    own = jnp.exp(new_score - top)
    denominator = jnp.sum(total * factor, axis=0) + own
    numerator = jnp.sum(sums * factor, axis=0) + own * own_ref[4:8]
    attention = (numerator / denominator).astype(jnp.bfloat16)
    out_ref[...] = jnp.broadcast_to(attention[None], out_ref.shape)


def merged_attention(
    queries, key_cache, value_cache, new_key, new_value, page_table, counts, offsets, groups
):
    requests = queries.shape[0]
    peers = lax.axis_size(SEQ)
    vmem = pl.BlockSpec(memory_space=pltpu.VMEM)
    hbm = pl.BlockSpec(memory_space=pltpu.HBM)
    half = (*value_cache.shape[:2], value_cache.shape[2] // 2)
    small = pltpu.CompilerParams(vmem_limit_bytes=8 << 20)

    def near(x):
        return pltpu.with_memory_space_constraint(x, pltpu.VMEM)

    def far(x):
        return pltpu.with_memory_space_constraint(x, pltpu.HBM)

    all_queries = lax.all_to_all(
        jnp.broadcast_to(queries[None], (peers, *queries.shape)), SEQ, 0, 0, tiled=True
    )
    keys, values, rows, own = pl.pallas_call(
        fetch_pages,
        out_shape=(
            pltpu.VMEM(key_cache.shape, key_cache.dtype),
            pltpu.VMEM(half, value_cache.dtype),
            pltpu.VMEM((3, 8, HD), jnp.int32),
            pltpu.VMEM((8, HD), jnp.float32),
        ),
        in_specs=[hbm] * 8,
        out_specs=(vmem,) * 4,
        scratch_shapes=[pltpu.SMEM((requests,), jnp.int32)] * 3
        + [pltpu.VMEM((requests, HD), jnp.bfloat16)] * 3
        + [pltpu.SemaphoreType.DMA((8,))],
        compiler_params=small,
    )(
        far(page_table[:, 0]), far(counts[:, 0]), far(offsets),
        far(queries), far(new_key), far(new_value), far(key_cache), far(value_cache),
    )
    blocks = pl.pallas_call(
        attend_pages,
        out_shape=pltpu.VMEM((HEADS, 8, HD), jnp.bfloat16),
        in_specs=[vmem, vmem, vmem, hbm, vmem],
        out_specs=vmem,
        scratch_shapes=[pltpu.VMEM(half, value_cache.dtype)]
        + [pltpu.VMEM((HEADS * requests, HD), jnp.float32)] * 3
        + [pltpu.SemaphoreType.DMA],
        compiler_params=small,
    )(
        near(all_queries.reshape(HEADS * requests, HD)),
        near(keys), near(values), far(value_cache), near(rows),
    )
    blocks = lax.all_to_all(blocks, SEQ, 0, 0, tiled=True)
    attention = pl.pallas_call(
        merge_blocks,
        out_shape=pltpu.VMEM((groups, requests, HD), jnp.bfloat16),
        in_specs=[vmem] * 2,
        out_specs=vmem,
        compiler_params=small,
    )(near(blocks), near(own))
    return attention


def on_device(
    queries, key_cache, value_cache, new_key, new_value, page_table, counts, offsets, w_out
):
    requests = queries.shape[0]
    peers = lax.axis_size(SEQ)
    groups = lax.axis_size("batch")
    attention = merged_attention(
        queries, key_cache, value_cache, new_key, new_value, page_table, counts, offsets, groups
    )
    attention = lax.all_to_all(attention, "batch", 0, 0, tiled=True)
    partial = jnp.dot(
        attention.reshape(groups * requests, HD), w_out, preferred_element_type=jnp.float32
    )
    partial = partial.reshape(peers, -1, partial.shape[1])
    partial = lax.all_to_all(partial, SEQ, 0, 0, tiled=True)
    return jnp.sum(partial, axis=0).astype(jnp.bfloat16)


def solution(mesh):
    torus = Mesh(mesh.devices.reshape(4, 8, mesh.shape["batch"]), ("seq_0", "seq_1", "batch"))
    in_specs = (
        P("batch", SEQ),
        P("batch", SEQ, None),
        P("batch", SEQ, None),
        P("batch", None),
        P("batch", None),
        P("batch", SEQ),
        P("batch", SEQ),
        P("batch"),
        P(SEQ, "batch"),
    )
    return jax.shard_map(
        on_device, mesh=torus, in_specs=in_specs, out_specs=P(SEQ, "batch"), check_vma=False
    )
```

```python
import jax
import jax.numpy as jnp
from jax import lax
from jax.experimental import pallas as pl
from jax.experimental.pallas import tpu as pltpu
from jax.sharding import PartitionSpec as P

HEADS = 32
KVH = 16
HD = 128
QSCALAR = 144
SCALE = QSCALAR ** (-0.5)
SEQ = "seq"
BATCH = "batch"
FIRST = 20
FLOOR = -1e30
UNROLL = 4


def by_request(row, values):
    request = row & 3
    picked = jnp.where(request == 0, values[0], values[1])
    return jnp.where(request >= 2, jnp.where(request == 2, values[2], values[3]), picked)


def exchange(x, axis, first):
    size = lax.axis_size(axis)
    order = [(first + i) % size for i in range(size)]
    return lax.all_to_all(x, axis, 0, 0, axis_index_groups=[order], tiled=True)


def fetch_pages(
    table_far, counts_far, offsets_far, q_far, new_key_far, new_value_far, k_far, v_far,
    k_ref, v_ref, rows_ref, own_ref,
    table_ref, counts_ref, offsets_ref, q_ref, new_key_ref, new_value_ref, arrived,
):
    place = lax.axis_index(SEQ)
    column = pl.multiple_of((place // (HEADS // KVH)) * HD, HD)
    half = v_ref.shape[2]
    loads = [
        pltpu.make_async_copy(source, target, arrived.at[i])
        for i, (source, target) in enumerate(
            (
                (table_far, table_ref),
                (counts_far, counts_ref),
                (offsets_far, offsets_ref),
                (q_far, q_ref),
                (new_key_far.at[:, pl.ds(column, HD)], new_key_ref),
                (new_value_far.at[:, pl.ds(column, HD)], new_value_ref),
                (k_far, k_ref),
                (v_far.at[:, :, pl.ds(0, half)], v_ref),
            )
        )
    ]
    for load in loads:
        load.start()
    row = lax.broadcasted_iota(jnp.int32, (8, HD), 0)
    for load in loads[:6]:
        load.wait()
    rows_ref[0] = by_request(row, [table_ref[r] for r in range(4)])
    rows_ref[1] = by_request(row, [counts_ref[r] for r in range(4)])
    rows_ref[2] = by_request(row, [offsets_ref[r] - place * HD for r in range(4)])
    key = new_key_ref[...].astype(jnp.float32)
    score = jnp.sum(q_ref[...].astype(jnp.float32) * key, axis=1, keepdims=True) * SCALE
    own_ref[0:4] = jnp.broadcast_to(score, (4, HD))
    own_ref[4:8] = new_value_ref[...].astype(jnp.float32)
    for load in loads[6:]:
        load.wait()


def attend_pages(
    q_ref, k_ref, v_ref, v_far, rows_ref, out_ref,
    later_ref, wide_ref, scores_ref, stats_ref, arrived,
):
    half = later_ref.shape[2]
    later = pltpu.make_async_copy(v_far.at[:, :, pl.ds(half, half)], later_ref, arrived)
    later.start()
    row = lax.broadcasted_iota(jnp.int32, (8, HD), 0)
    lane = lax.broadcasted_iota(jnp.int32, (8, HD), 1)
    slot = rows_ref[0]

    def apart(x):
        return jnp.concatenate(
            [jnp.where(slot == i, x, 0.0) for i in range(4)], axis=1
        ).astype(jnp.bfloat16)

    wide_ref[...] = q_ref[...].astype(jnp.float32)

    def score(i, carry):
        for j in range(UNROLL):
            turn = i * UNROLL + j
            k = (turn + FIRST // 2) % KVH
            rows = pl.ds(pl.multiple_of(turn * 8, 8), 8)
            cols = pl.ds(pl.multiple_of(k * HD, HD), HD)
            keys = jnp.concatenate([k_ref[i, :, cols] for i in range(4)], axis=1)
            scores_ref[rows] = lax.dot_general(
                apart(wide_ref[rows]),
                keys,
                (((1,), (1,)), ((), ())),
                preferred_element_type=jnp.float32,
            )
        return carry

    lax.fori_loop(0, KVH // UNROLL, score, 0)
    live = ((lane < rows_ref[1]) & (lane >= rows_ref[2]))[None]
    scores = scores_ref[...].reshape(KVH, 8, HD) * SCALE
    peak = jnp.max(jnp.where(live, scores, FLOOR), axis=2, keepdims=True)
    weights = jnp.where(live, jnp.exp(scores - peak), 0.0)
    mark = peak.astype(jnp.bfloat16).astype(jnp.float32)
    shift = jnp.exp(jnp.minimum(peak - mark, 64.0))
    total = jnp.sum(weights, axis=2, keepdims=True) * shift
    coarse = total.astype(jnp.bfloat16).astype(jnp.float32)
    stats = jnp.where(lane == 1, coarse, jnp.where(lane == 2, total - coarse, shift))
    scores_ref[...] = weights.reshape(KVH * 8, HD)
    stats_ref[...] = jnp.where(lane == 0, mark, stats).reshape(KVH * 8, HD)

    def value(held, base):
        def step(i, carry):
            for j in range(UNROLL):
                k = i * UNROLL + j
                turn = (base + k + KVH - FIRST // 2) % KVH
                rows = pl.ds(pl.multiple_of(turn * 8, 8), 8)
                cols = pl.ds(pl.multiple_of(k * HD, HD), HD)
                values = jnp.concatenate([held[i, :, cols] for i in range(4)], axis=0)
                sums = jnp.dot(
                    apart(scores_ref[rows]), values, preferred_element_type=jnp.float32
                )
                stats = stats_ref[rows]
                sums = sums * stats[:, 3:4]
                even = jnp.where(row < 4, sums, pltpu.roll(stats, 4, 0))
                odd = jnp.where(row < 4, pltpu.roll(sums, 4, 0), stats)
                out_ref[2 * turn] = even.astype(jnp.bfloat16)
                out_ref[2 * turn + 1] = odd.astype(jnp.bfloat16)
            return carry

        return step

    lax.fori_loop(0, KVH // 2 // UNROLL, value(v_ref, 0), 0)
    later.wait()
    lax.fori_loop(0, KVH // 2 // UNROLL, value(later_ref, KVH // 2), 0)


def merge_blocks(blocks_ref, own_ref, out_ref):
    blocks = blocks_ref[...].astype(jnp.float32)
    sums = blocks[:, 0:4, :]
    mark = blocks[:, 4:8, 0:1]
    total = blocks[:, 4:8, 1:2] + blocks[:, 4:8, 2:3]
    new_score = own_ref[0:4, 0:1]
    top = jnp.maximum(jnp.max(mark, axis=0), new_score)
    factor = jnp.exp(mark - top[None])
    own = jnp.exp(new_score - top)
    denominator = jnp.sum(total * factor, axis=0) + own
    numerator = jnp.sum(sums * factor, axis=0) + own * own_ref[4:8]
    attention = (numerator / denominator).astype(jnp.bfloat16)
    out_ref[...] = jnp.broadcast_to(attention[None], out_ref.shape)


def merged_attention(
    queries, key_cache, value_cache, new_key, new_value, page_table, counts, offsets, groups
):
    requests = queries.shape[0]
    peers = lax.axis_size(SEQ)
    vmem = pl.BlockSpec(memory_space=pltpu.VMEM)
    hbm = pl.BlockSpec(memory_space=pltpu.HBM)
    half = (*value_cache.shape[:2], value_cache.shape[2] // 2)
    small = pltpu.CompilerParams(vmem_limit_bytes=8 << 20)

    def near(x):
        return pltpu.with_memory_space_constraint(x, pltpu.VMEM)

    def far(x):
        return pltpu.with_memory_space_constraint(x, pltpu.HBM)

    all_queries = exchange(jnp.broadcast_to(queries[None], (peers, *queries.shape)), SEQ, FIRST)
    keys, values, rows, own = pl.pallas_call(
        fetch_pages,
        out_shape=(
            pltpu.VMEM(key_cache.shape, key_cache.dtype),
            pltpu.VMEM(half, value_cache.dtype),
            pltpu.VMEM((3, 8, HD), jnp.int32),
            pltpu.VMEM((8, HD), jnp.float32),
        ),
        in_specs=[hbm] * 8,
        out_specs=(vmem,) * 4,
        scratch_shapes=[pltpu.SMEM((requests,), jnp.int32)] * 3
        + [pltpu.VMEM((requests, HD), jnp.bfloat16)] * 3
        + [pltpu.SemaphoreType.DMA((8,))],
        compiler_params=small,
    )(
        far(page_table[:, 0]), far(counts[:, 0]), far(offsets),
        far(queries), far(new_key), far(new_value), far(key_cache), far(value_cache),
    )
    blocks = pl.pallas_call(
        attend_pages,
        out_shape=pltpu.VMEM((HEADS, 8, HD), jnp.bfloat16),
        in_specs=[vmem, vmem, vmem, hbm, vmem],
        out_specs=vmem,
        scratch_shapes=[pltpu.VMEM(half, value_cache.dtype)]
        + [pltpu.VMEM((HEADS * requests, HD), jnp.float32)] * 3
        + [pltpu.SemaphoreType.DMA],
        compiler_params=small,
    )(
        near(all_queries.reshape(HEADS * requests, HD)),
        near(keys), near(values), far(value_cache), near(rows),
    )
    blocks = exchange(blocks, SEQ, FIRST)
    attention = pl.pallas_call(
        merge_blocks,
        out_shape=pltpu.VMEM((groups, requests, HD), jnp.bfloat16),
        in_specs=[vmem] * 2,
        out_specs=vmem,
        compiler_params=small,
    )(near(blocks), near(own))
    return attention


def on_device(
    queries, key_cache, value_cache, new_key, new_value, page_table, counts, offsets, w_out
):
    requests = queries.shape[0]
    peers = lax.axis_size(SEQ)
    groups = lax.axis_size(BATCH)
    attention = merged_attention(
        queries, key_cache, value_cache, new_key, new_value, page_table, counts, offsets, groups
    )
    attention = exchange(attention, BATCH, FIRST // 2)
    partial = jnp.dot(
        attention.reshape(groups * requests, HD), w_out, preferred_element_type=jnp.float32
    )
    partial = partial.reshape(peers, -1, partial.shape[1])
    partial = exchange(partial, SEQ, FIRST)
    return jnp.sum(partial, axis=0).astype(jnp.bfloat16)


def solution(mesh):
    in_specs = (
        P(BATCH, SEQ),
        P(BATCH, SEQ, None),
        P(BATCH, SEQ, None),
        P(BATCH, None),
        P(BATCH, None),
        P(BATCH, SEQ),
        P(BATCH, SEQ),
        P(BATCH),
        P(SEQ, BATCH),
    )
    return jax.shard_map(
        on_device, mesh=mesh, in_specs=in_specs, out_specs=P(SEQ, BATCH), check_vma=False
    )
```

```python
import jax
import jax.numpy as jnp
from jax import lax
from jax.experimental import pallas as pl
from jax.experimental.pallas import tpu as pltpu
from jax.sharding import PartitionSpec as P

HEADS = 32
KVH = 16
HD = 128
QSCALAR = 144
SCALE = QSCALAR ** (-0.5)
SEQ = "seq"
BATCH = "batch"
PAIRS = (10, 0, 3, 4, 1, 12, 7, 15, 8, 11, 5, 2, 13, 9, 6, 14)
FLOOR = -1e30
TURNS = tuple(PAIRS.index(k) for k in range(KVH))
ORDER = tuple(2 * k + i for k in PAIRS for i in range(2))
UNROLL = 8
STATS = 3


def by_request(row, values):
    request = row & 3
    picked = jnp.where(request == 0, values[0], values[1])
    return jnp.where(request >= 2, jnp.where(request == 2, values[2], values[3]), picked)


def exchange(x, axis, order):
    return lax.all_to_all(x, axis, 0, 0, axis_index_groups=[list(order)], tiled=True)


def looked_up(table, i, j):
    packed = sum(value << (4 * n) for n, value in enumerate(table[j::UNROLL]))
    return lax.shift_right_logical(jnp.int32(packed), jnp.int32(4) * i) & 15


def fetch_pages(
    table_far, counts_far, offsets_far, q_far, new_key_far, new_value_far, k_far, v_far,
    k_ref, v_ref, rows_ref, own_ref,
    table_ref, counts_ref, offsets_ref, q_ref, new_key_ref, new_value_ref, arrived,
):
    place = lax.axis_index(SEQ)
    column = pl.multiple_of((place // (HEADS // KVH)) * HD, HD)
    half = v_ref.shape[2]
    loads = [
        pltpu.make_async_copy(source, target, arrived.at[i])
        for i, (source, target) in enumerate(
            (
                (table_far, table_ref),
                (counts_far, counts_ref),
                (offsets_far, offsets_ref),
                (q_far, q_ref),
                (new_key_far.at[:, pl.ds(column, HD)], new_key_ref),
                (new_value_far.at[:, pl.ds(column, HD)], new_value_ref),
                (k_far, k_ref),
                (v_far.at[:, :, pl.ds(0, half)], v_ref),
            )
        )
    ]
    for load in loads:
        load.start()
    row = lax.broadcasted_iota(jnp.int32, (8, HD), 0)
    for load in loads[:6]:
        load.wait()
    rows_ref[0] = by_request(row, [table_ref[r] for r in range(4)])
    rows_ref[1] = by_request(row, [counts_ref[r] for r in range(4)])
    rows_ref[2] = by_request(row, [offsets_ref[r] - place * HD for r in range(4)])
    key = new_key_ref[...].astype(jnp.float32)
    score = jnp.sum(q_ref[...].astype(jnp.float32) * key, axis=1, keepdims=True) * SCALE
    own_ref[0:4] = jnp.broadcast_to(score, (4, HD))
    own_ref[4:8] = new_value_ref[...].astype(jnp.float32)
    for load in loads[6:]:
        load.wait()


def attend_pages(
    q_ref, k_ref, v_ref, v_far, rows_ref, out_ref,
    later_ref, wide_ref, scores_ref, stats_ref, arrived,
):
    half = later_ref.shape[2]
    later = pltpu.make_async_copy(v_far.at[:, :, pl.ds(half, half)], later_ref, arrived)
    later.start()
    row = lax.broadcasted_iota(jnp.int32, (8, HD), 0)
    lane = lax.broadcasted_iota(jnp.int32, (8, HD), 1)
    slot = rows_ref[0]

    def apart(x):
        return jnp.concatenate(
            [jnp.where(slot == i, x, 0.0) for i in range(4)], axis=1
        ).astype(jnp.bfloat16)

    wide_ref[...] = q_ref[...].astype(jnp.float32)

    def score(i, carry):
        for j in range(UNROLL):
            turn = i * UNROLL + j
            k = looked_up(PAIRS, i, j)
            rows = pl.ds(pl.multiple_of(turn * 8, 8), 8)
            cols = pl.ds(pl.multiple_of(k * HD, HD), HD)
            keys = jnp.concatenate([k_ref[i, :, cols] for i in range(4)], axis=1)
            scores_ref[rows] = lax.dot_general(
                apart(wide_ref[rows]),
                keys,
                (((1,), (1,)), ((), ())),
                preferred_element_type=jnp.float32,
            )
        return carry

    lax.fori_loop(0, KVH // UNROLL, score, 0)
    live = ((lane < rows_ref[1]) & (lane >= rows_ref[2]))[None]
    scores = scores_ref[...].reshape(KVH, 8, HD) * SCALE
    peak = jnp.max(jnp.where(live, scores, FLOOR), axis=2, keepdims=True)
    weights = jnp.where(live, jnp.exp(scores - peak), 0.0)
    mark = peak.astype(jnp.bfloat16).astype(jnp.float32)
    shift = jnp.exp(jnp.minimum(peak - mark, 64.0))
    total = jnp.sum(weights, axis=2, keepdims=True) * shift
    coarse = total.astype(jnp.bfloat16).astype(jnp.float32)
    stats = jnp.where(lane == 1, coarse, jnp.where(lane == 2, total - coarse, shift))
    scores_ref[...] = weights.reshape(KVH * 8, HD)
    stats_ref[...] = jnp.where(lane == 0, mark, stats).reshape(KVH * 8, HD)

    def value(held, base):
        def step(i, carry):
            for j in range(UNROLL):
                k = i * UNROLL + j
                turn = looked_up(TURNS[base : base + KVH // 2], i, j)
                rows = pl.ds(pl.multiple_of(turn * 8, 8), 8)
                cols = pl.ds(pl.multiple_of(k * HD, HD), HD)
                values = jnp.concatenate([held[i, :, cols] for i in range(4)], axis=0)
                sums = jnp.dot(
                    apart(scores_ref[rows]), values, preferred_element_type=jnp.float32
                )
                stats = stats_ref[rows]
                sums = sums * stats[:, 3:4]
                rest = sums - sums.astype(jnp.bfloat16).astype(jnp.float32)
                rest = jnp.where(lane < STATS, stats, rest)
                even = jnp.where(row < 4, sums, pltpu.roll(rest, 4, 0))
                odd = jnp.where(row < 4, pltpu.roll(sums, 4, 0), rest)
                out_ref[2 * turn] = even.astype(jnp.bfloat16)
                out_ref[2 * turn + 1] = odd.astype(jnp.bfloat16)
            return carry

        return step

    lax.fori_loop(0, KVH // 2 // UNROLL, value(v_ref, 0), 0)
    later.wait()
    lax.fori_loop(0, KVH // 2 // UNROLL, value(later_ref, KVH // 2), 0)


def merge_blocks(blocks_ref, own_ref, out_ref):
    blocks = blocks_ref[...].astype(jnp.float32)
    lane = lax.broadcasted_iota(jnp.int32, (4, HD), 1)
    sums = blocks[:, 0:4, :] + jnp.where(lane < STATS, 0.0, blocks[:, 4:8, :])
    mark = blocks[:, 4:8, 0:1]
    total = blocks[:, 4:8, 1:2] + blocks[:, 4:8, 2:3]
    new_score = own_ref[0:4, 0:1]
    top = jnp.maximum(jnp.max(mark, axis=0), new_score)
    factor = jnp.exp(mark - top[None])
    own = jnp.exp(new_score - top)
    denominator = jnp.sum(total * factor, axis=0) + own
    numerator = jnp.sum(sums * factor, axis=0) + own * own_ref[4:8]
    attention = (numerator / denominator).astype(jnp.bfloat16)
    out_ref[...] = jnp.broadcast_to(attention[None], out_ref.shape)


def merged_attention(
    queries, key_cache, value_cache, new_key, new_value, page_table, counts, offsets, groups
):
    requests = queries.shape[0]
    peers = lax.axis_size(SEQ)
    vmem = pl.BlockSpec(memory_space=pltpu.VMEM)
    hbm = pl.BlockSpec(memory_space=pltpu.HBM)
    half = (*value_cache.shape[:2], value_cache.shape[2] // 2)
    small = pltpu.CompilerParams(vmem_limit_bytes=8 << 20)

    def near(x):
        return pltpu.with_memory_space_constraint(x, pltpu.VMEM)

    def far(x):
        return pltpu.with_memory_space_constraint(x, pltpu.HBM)

    all_queries = exchange(jnp.broadcast_to(queries[None], (peers, *queries.shape)), SEQ, ORDER)
    keys, values, rows, own = pl.pallas_call(
        fetch_pages,
        out_shape=(
            pltpu.VMEM(key_cache.shape, key_cache.dtype),
            pltpu.VMEM(half, value_cache.dtype),
            pltpu.VMEM((3, 8, HD), jnp.int32),
            pltpu.VMEM((8, HD), jnp.float32),
        ),
        in_specs=[hbm] * 8,
        out_specs=(vmem,) * 4,
        scratch_shapes=[pltpu.SMEM((requests,), jnp.int32)] * 3
        + [pltpu.VMEM((requests, HD), jnp.bfloat16)] * 3
        + [pltpu.SemaphoreType.DMA((8,))],
        compiler_params=small,
    )(
        far(page_table[:, 0]), far(counts[:, 0]), far(offsets),
        far(queries), far(new_key), far(new_value), far(key_cache), far(value_cache),
    )
    blocks = pl.pallas_call(
        attend_pages,
        out_shape=pltpu.VMEM((HEADS, 8, HD), jnp.bfloat16),
        in_specs=[vmem, vmem, vmem, hbm, vmem],
        out_specs=vmem,
        scratch_shapes=[pltpu.VMEM(half, value_cache.dtype)]
        + [pltpu.VMEM((HEADS * requests, HD), jnp.float32)] * 3
        + [pltpu.SemaphoreType.DMA],
        compiler_params=small,
    )(
        near(all_queries.reshape(HEADS * requests, HD)),
        near(keys), near(values), far(value_cache), near(rows),
    )
    blocks = exchange(blocks, SEQ, ORDER)
    attention = pl.pallas_call(
        merge_blocks,
        out_shape=pltpu.VMEM((groups, requests, HD), jnp.bfloat16),
        in_specs=[vmem] * 2,
        out_specs=vmem,
        compiler_params=small,
    )(near(blocks), near(own))
    return attention


def on_device(
    queries, key_cache, value_cache, new_key, new_value, page_table, counts, offsets, w_out
):
    requests = queries.shape[0]
    peers = lax.axis_size(SEQ)
    groups = lax.axis_size(BATCH)
    attention = merged_attention(
        queries, key_cache, value_cache, new_key, new_value, page_table, counts, offsets, groups
    )
    attention = exchange(attention, BATCH, PAIRS)
    partial = jnp.dot(
        attention.reshape(groups * requests, HD), w_out, preferred_element_type=jnp.float32
    )
    partial = partial.astype(jnp.bfloat16).reshape(peers, -1, partial.shape[1])
    partial = exchange(partial, SEQ, ORDER)
    return jnp.sum(partial.astype(jnp.float32), axis=0).astype(jnp.bfloat16)


def solution(mesh):
    in_specs = (
        P(BATCH, SEQ),
        P(BATCH, SEQ, None),
        P(BATCH, SEQ, None),
        P(BATCH, None),
        P(BATCH, None),
        P(BATCH, SEQ),
        P(BATCH, SEQ),
        P(BATCH),
        P(SEQ, BATCH),
    )
    return jax.shard_map(
        on_device, mesh=mesh, in_specs=in_specs, out_specs=P(SEQ, BATCH), check_vma=False
    )
```

```python
import jax
import jax.numpy as jnp
from jax import lax
from jax.experimental import pallas as pl
from jax.experimental.pallas import tpu as pltpu
from jax.sharding import PartitionSpec as P

HEADS = 32
KVH = 16
HD = 128
QSCALAR = 144
SCALE = QSCALAR ** (-0.5)
SEQ = "seq"
BATCH = "batch"
PAIRS = (10, 6, 7, 8, 9, 4, 5, 15, 11, 2, 3, 12, 13, 0, 1, 14)
SWAP = 7
FLOOR = -1e30
TURNS = tuple(PAIRS.index(k) for k in range(KVH))
GROUPS = (PAIRS[SWAP], *PAIRS[1:SWAP], PAIRS[0], *PAIRS[SWAP + 1 :])
ORDER = tuple(2 * k + i for k in PAIRS for i in range(2))
UNROLL = 8
STATS = 3


def by_request(row, values):
    request = row & 3
    picked = jnp.where(request == 0, values[0], values[1])
    return jnp.where(request >= 2, jnp.where(request == 2, values[2], values[3]), picked)


def exchange(x, axis, order):
    return lax.all_to_all(x, axis, 0, 0, axis_index_groups=[list(order)], tiled=True)


def looked_up(table, i, j):
    packed = sum(value << (4 * n) for n, value in enumerate(table[j::UNROLL]))
    return lax.shift_right_logical(jnp.int32(packed), jnp.int32(4) * i) & 15


def fetch_pages(
    table_far, counts_far, offsets_far, q_far, new_key_far, new_value_far, k_far, v_far,
    spread_ref, k_ref, v_ref, rows_ref, own_ref,
    table_ref, counts_ref, offsets_ref, q_ref, new_key_ref, new_value_ref, arrived,
):
    place = lax.axis_index(SEQ)
    column = pl.multiple_of((place // (HEADS // KVH)) * HD, HD)
    half = v_ref.shape[2]
    loads = [
        pltpu.make_async_copy(source, target, arrived.at[i])
        for i, (source, target) in enumerate(
            (
                (q_far, q_ref),
                (table_far, table_ref),
                (counts_far, counts_ref),
                (offsets_far, offsets_ref),
                (new_key_far.at[:, pl.ds(column, HD)], new_key_ref),
                (new_value_far.at[:, pl.ds(column, HD)], new_value_ref),
                (k_far, k_ref),
                (v_far.at[:, :, pl.ds(0, half)], v_ref),
            )
        )
    ]
    for load in loads:
        load.start()
    row = lax.broadcasted_iota(jnp.int32, (8, HD), 0)
    for load in loads[:6]:
        load.wait()
    spread_ref[...] = jnp.broadcast_to(q_ref[...][None], spread_ref.shape)
    rows_ref[0] = by_request(row, [table_ref[r] for r in range(4)])
    rows_ref[1] = by_request(row, [counts_ref[r] for r in range(4)])
    rows_ref[2] = by_request(row, [offsets_ref[r] - place * HD for r in range(4)])
    key = new_key_ref[...].astype(jnp.float32)
    score = jnp.sum(q_ref[...].astype(jnp.float32) * key, axis=1, keepdims=True) * SCALE
    own_ref[0:4] = jnp.broadcast_to(score, (4, HD))
    own_ref[4:8] = new_value_ref[...].astype(jnp.float32)
    for load in loads[6:]:
        load.wait()


def attend_pages(
    q_ref, k_ref, v_ref, v_far, rows_ref, out_ref,
    later_ref, wide_ref, scores_ref, stats_ref, arrived,
):
    half = later_ref.shape[2]
    later = pltpu.make_async_copy(v_far.at[:, :, pl.ds(half, half)], later_ref, arrived)
    later.start()
    row = lax.broadcasted_iota(jnp.int32, (8, HD), 0)
    lane = lax.broadcasted_iota(jnp.int32, (8, HD), 1)
    slot = rows_ref[0]

    def apart(x):
        return jnp.concatenate(
            [jnp.where(slot == i, x, 0.0) for i in range(4)], axis=1
        ).astype(jnp.bfloat16)

    wide_ref[...] = q_ref[...].astype(jnp.float32)

    def score(i, carry):
        for j in range(UNROLL):
            turn = i * UNROLL + j
            k = looked_up(PAIRS, i, j)
            rows = pl.ds(pl.multiple_of(turn * 8, 8), 8)
            cols = pl.ds(pl.multiple_of(k * HD, HD), HD)
            keys = jnp.concatenate([k_ref[i, :, cols] for i in range(4)], axis=1)
            scores_ref[rows] = lax.dot_general(
                apart(wide_ref[rows]),
                keys,
                (((1,), (1,)), ((), ())),
                preferred_element_type=jnp.float32,
            )
        return carry

    lax.fori_loop(0, KVH // UNROLL, score, 0)
    live = ((lane < rows_ref[1]) & (lane >= rows_ref[2]))[None]
    scores = scores_ref[...].reshape(KVH, 8, HD) * SCALE
    peak = jnp.max(jnp.where(live, scores, FLOOR), axis=2, keepdims=True)
    weights = jnp.where(live, jnp.exp(scores - peak), 0.0)
    mark = peak.astype(jnp.bfloat16).astype(jnp.float32)
    shift = jnp.exp(jnp.minimum(peak - mark, 64.0))
    total = jnp.sum(weights, axis=2, keepdims=True) * shift
    coarse = total.astype(jnp.bfloat16).astype(jnp.float32)
    stats = jnp.where(lane == 1, coarse, jnp.where(lane == 2, total - coarse, shift))
    scores_ref[...] = weights.reshape(KVH * 8, HD)
    stats_ref[...] = jnp.where(lane == 0, mark, stats).reshape(KVH * 8, HD)

    def value(held, base):
        def step(i, carry):
            for j in range(UNROLL):
                k = i * UNROLL + j
                turn = looked_up(TURNS[base : base + KVH // 2], i, j)
                rows = pl.ds(pl.multiple_of(turn * 8, 8), 8)
                cols = pl.ds(pl.multiple_of(k * HD, HD), HD)
                values = jnp.concatenate([held[i, :, cols] for i in range(4)], axis=0)
                sums = jnp.dot(
                    apart(scores_ref[rows]), values, preferred_element_type=jnp.float32
                )
                stats = stats_ref[rows]
                sums = sums * stats[:, 3:4]
                rest = sums - sums.astype(jnp.bfloat16).astype(jnp.float32)
                rest = jnp.where(lane < STATS, stats, rest)
                even = jnp.where(row < 4, sums, pltpu.roll(rest, 4, 0))
                odd = jnp.where(row < 4, pltpu.roll(sums, 4, 0), rest)
                out_ref[2 * turn] = even.astype(jnp.bfloat16)
                out_ref[2 * turn + 1] = odd.astype(jnp.bfloat16)
            return carry

        return step

    lax.fori_loop(0, KVH // 2 // UNROLL, value(v_ref, 0), 0)
    later.wait()
    lax.fori_loop(0, KVH // 2 // UNROLL, value(later_ref, KVH // 2), 0)


def merge_blocks(blocks_ref, own_ref, out_ref):
    blocks = blocks_ref[...].astype(jnp.float32)
    lane = lax.broadcasted_iota(jnp.int32, (4, HD), 1)
    sums = blocks[:, 0:4, :] + jnp.where(lane < STATS, 0.0, blocks[:, 4:8, :])
    mark = blocks[:, 4:8, 0:1]
    total = blocks[:, 4:8, 1:2] + blocks[:, 4:8, 2:3]
    new_score = own_ref[0:4, 0:1]
    top = jnp.maximum(jnp.max(mark, axis=0), new_score)
    factor = jnp.exp(mark - top[None])
    own = jnp.exp(new_score - top)
    denominator = jnp.sum(total * factor, axis=0) + own
    numerator = jnp.sum(sums * factor, axis=0) + own * own_ref[4:8]
    attention = (numerator / denominator).astype(jnp.bfloat16)
    out_ref[...] = jnp.broadcast_to(attention[None], out_ref.shape)


def project(attention_ref, w_ref, out_ref):
    blocks = attention_ref[...].astype(jnp.float32)
    rows = jnp.concatenate([blocks[GROUPS.index(k)] for k in PAIRS]).astype(jnp.bfloat16)
    out_ref[...] = lax.dot_general(
        rows, w_ref[...], (((1,), (1,)), ((), ())), preferred_element_type=jnp.float32
    ).astype(jnp.bfloat16)


def merged_attention(
    queries, key_cache, value_cache, new_key, new_value, page_table, counts, offsets, groups
):
    requests = queries.shape[0]
    peers = lax.axis_size(SEQ)
    vmem = pl.BlockSpec(memory_space=pltpu.VMEM)
    hbm = pl.BlockSpec(memory_space=pltpu.HBM)
    half = (*value_cache.shape[:2], value_cache.shape[2] // 2)
    small = pltpu.CompilerParams(vmem_limit_bytes=8 << 20)

    def near(x):
        return pltpu.with_memory_space_constraint(x, pltpu.VMEM)

    def far(x):
        return pltpu.with_memory_space_constraint(x, pltpu.HBM)

    spread, keys, values, rows, own = pl.pallas_call(
        fetch_pages,
        out_shape=(
            pltpu.VMEM((peers, *queries.shape), queries.dtype),
            pltpu.VMEM(key_cache.shape, key_cache.dtype),
            pltpu.VMEM(half, value_cache.dtype),
            pltpu.VMEM((3, 8, HD), jnp.int32),
            pltpu.VMEM((8, HD), jnp.float32),
        ),
        in_specs=[hbm] * 8,
        out_specs=(vmem,) * 5,
        scratch_shapes=[pltpu.SMEM((requests,), jnp.int32)] * 3
        + [pltpu.VMEM((requests, HD), jnp.bfloat16)] * 3
        + [pltpu.SemaphoreType.DMA((8,))],
        compiler_params=small,
    )(
        far(page_table[:, 0]), far(counts[:, 0]), far(offsets),
        far(queries), far(new_key), far(new_value), far(key_cache), far(value_cache),
    )
    all_queries = exchange(spread, SEQ, ORDER)
    blocks = pl.pallas_call(
        attend_pages,
        out_shape=pltpu.VMEM((HEADS, 8, HD), jnp.bfloat16),
        in_specs=[vmem, vmem, vmem, hbm, vmem],
        out_specs=vmem,
        scratch_shapes=[pltpu.VMEM(half, value_cache.dtype)]
        + [pltpu.VMEM((HEADS * requests, HD), jnp.float32)] * 3
        + [pltpu.SemaphoreType.DMA],
        compiler_params=small,
    )(
        near(all_queries.reshape(HEADS * requests, HD)),
        near(keys), near(values), far(value_cache), near(rows),
    )
    blocks = exchange(blocks, SEQ, ORDER)
    attention = pl.pallas_call(
        merge_blocks,
        out_shape=pltpu.VMEM((groups, requests, HD), jnp.bfloat16),
        in_specs=[vmem] * 2,
        out_specs=vmem,
        compiler_params=small,
    )(near(blocks), near(own))
    return attention


def on_device(
    queries, key_cache, value_cache, new_key, new_value, page_table, counts, offsets, w_out
):
    requests = queries.shape[0]
    peers = lax.axis_size(SEQ)
    groups = lax.axis_size(BATCH)
    attention = merged_attention(
        queries, key_cache, value_cache, new_key, new_value, page_table, counts, offsets, groups
    )
    attention = exchange(attention, BATCH, GROUPS)
    vmem = pl.BlockSpec(memory_space=pltpu.VMEM)
    partial = pl.pallas_call(
        project,
        out_shape=pltpu.VMEM((groups * requests, w_out.shape[1]), jnp.bfloat16),
        in_specs=[vmem] * 2,
        out_specs=vmem,
        compiler_params=pltpu.CompilerParams(vmem_limit_bytes=8 << 20),
    )(
        pltpu.with_memory_space_constraint(attention, pltpu.VMEM),
        pltpu.with_memory_space_constraint(w_out.T, pltpu.VMEM),
    )
    partial = partial.reshape(peers, -1, partial.shape[1])
    partial = exchange(partial, SEQ, ORDER)
    return jnp.sum(partial.astype(jnp.float32), axis=0).astype(jnp.bfloat16)


def solution(mesh):
    in_specs = (
        P(BATCH, SEQ),
        P(BATCH, SEQ, None),
        P(BATCH, SEQ, None),
        P(BATCH, None),
        P(BATCH, None),
        P(BATCH, SEQ),
        P(BATCH, SEQ),
        P(BATCH),
        P(SEQ, BATCH),
    )
    return jax.shard_map(
        on_device, mesh=mesh, in_specs=in_specs, out_specs=P(SEQ, BATCH), check_vma=False
    )
```

```python
import jax
import jax.numpy as jnp
from jax import lax
from jax.experimental import pallas as pl
from jax.experimental.pallas import tpu as pltpu
from jax.sharding import PartitionSpec as P

HEADS = 32
KVH = 16
HD = 128
QSCALAR = 144
SCALE = QSCALAR ** (-0.5)
SEQ = "seq"
BATCH = "batch"
PAIRS = (10, 0, 3, 4, 1, 12, 7, 15, 8, 11, 5, 2, 13, 9, 6, 14)
SWAP = 7
FLOOR = -1e30
TURNS = tuple(PAIRS.index(k) for k in range(KVH))
GROUPS = (PAIRS[SWAP], *PAIRS[1:SWAP], PAIRS[0], *PAIRS[SWAP + 1 :])
ORDER = tuple(2 * k + i for k in PAIRS for i in range(2))
UNROLL = 8
STATS = 3


def by_request(row, values):
    request = row & 3
    picked = jnp.where(request == 0, values[0], values[1])
    return jnp.where(request >= 2, jnp.where(request == 2, values[2], values[3]), picked)


def exchange(x, axis, order):
    return lax.all_to_all(x, axis, 0, 0, axis_index_groups=[list(order)], tiled=True)


def looked_up(table, i, j):
    packed = sum(value << (4 * n) for n, value in enumerate(table[j::UNROLL]))
    return lax.shift_right_logical(jnp.int32(packed), jnp.int32(4) * i) & 15


def fetch_pages(
    table_far, counts_far, offsets_far, q_far, new_key_far, new_value_far, k_far, v_far,
    spread_ref, k_ref, v_ref, rows_ref, own_ref,
    table_ref, counts_ref, offsets_ref, q_ref, new_key_ref, new_value_ref, arrived,
):
    place = lax.axis_index(SEQ)
    column = pl.multiple_of((place // (HEADS // KVH)) * HD, HD)
    half = v_ref.shape[2]
    loads = [
        pltpu.make_async_copy(source, target, arrived.at[i])
        for i, (source, target) in enumerate(
            (
                (q_far, q_ref),
                (table_far, table_ref),
                (counts_far, counts_ref),
                (offsets_far, offsets_ref),
                (new_key_far.at[:, pl.ds(column, HD)], new_key_ref),
                (new_value_far.at[:, pl.ds(column, HD)], new_value_ref),
                (k_far, k_ref),
                (v_far.at[:, :, pl.ds(0, half)], v_ref),
            )
        )
    ]
    for load in loads:
        load.start()
    row = lax.broadcasted_iota(jnp.int32, (8, HD), 0)
    for load in loads[:6]:
        load.wait()
    spread_ref[...] = jnp.broadcast_to(q_ref[...][None], spread_ref.shape)
    rows_ref[0] = by_request(row, [table_ref[r] for r in range(4)])
    rows_ref[1] = by_request(row, [counts_ref[r] for r in range(4)])
    rows_ref[2] = by_request(row, [offsets_ref[r] - place * HD for r in range(4)])
    key = new_key_ref[...].astype(jnp.float32)
    score = jnp.sum(q_ref[...].astype(jnp.float32) * key, axis=1, keepdims=True) * SCALE
    own_ref[0:4] = jnp.broadcast_to(score, (4, HD))
    own_ref[4:8] = new_value_ref[...].astype(jnp.float32)
    for load in loads[6:]:
        load.wait()


def attend_pages(
    q_ref, k_ref, v_ref, v_far, rows_ref, out_ref,
    later_ref, wide_ref, scores_ref, stats_ref, arrived,
):
    half = later_ref.shape[2]
    later = pltpu.make_async_copy(v_far.at[:, :, pl.ds(half, half)], later_ref, arrived)
    later.start()
    row = lax.broadcasted_iota(jnp.int32, (8, HD), 0)
    lane = lax.broadcasted_iota(jnp.int32, (8, HD), 1)
    slot = rows_ref[0]

    def apart(x):
        return jnp.concatenate(
            [jnp.where(slot == i, x, 0.0) for i in range(4)], axis=1
        ).astype(jnp.bfloat16)

    wide_ref[...] = q_ref[...].astype(jnp.float32)

    def score(i, carry):
        for j in range(UNROLL):
            turn = i * UNROLL + j
            k = looked_up(PAIRS, i, j)
            rows = pl.ds(pl.multiple_of(turn * 8, 8), 8)
            cols = pl.ds(pl.multiple_of(k * HD, HD), HD)
            keys = jnp.concatenate([k_ref[i, :, cols] for i in range(4)], axis=1)
            scores_ref[rows] = lax.dot_general(
                apart(wide_ref[rows]),
                keys,
                (((1,), (1,)), ((), ())),
                preferred_element_type=jnp.float32,
            )
        return carry

    lax.fori_loop(0, KVH // UNROLL, score, 0)
    live = ((lane < rows_ref[1]) & (lane >= rows_ref[2]))[None]
    scores = scores_ref[...].reshape(KVH, 8, HD) * SCALE
    peak = jnp.max(jnp.where(live, scores, FLOOR), axis=2, keepdims=True)
    weights = jnp.where(live, jnp.exp(scores - peak), 0.0)
    mark = peak.astype(jnp.bfloat16).astype(jnp.float32)
    shift = jnp.exp(jnp.minimum(peak - mark, 64.0))
    total = jnp.sum(weights, axis=2, keepdims=True) * shift
    coarse = total.astype(jnp.bfloat16).astype(jnp.float32)
    stats = jnp.where(lane == 1, coarse, jnp.where(lane == 2, total - coarse, shift))
    scores_ref[...] = weights.reshape(KVH * 8, HD)
    stats_ref[...] = jnp.where(lane == 0, mark, stats).reshape(KVH * 8, HD)

    def value(held, base):
        def step(i, carry):
            for j in range(UNROLL):
                k = i * UNROLL + j
                turn = looked_up(TURNS[base : base + KVH // 2], i, j)
                rows = pl.ds(pl.multiple_of(turn * 8, 8), 8)
                cols = pl.ds(pl.multiple_of(k * HD, HD), HD)
                values = jnp.concatenate([held[i, :, cols] for i in range(4)], axis=0)
                sums = jnp.dot(
                    apart(scores_ref[rows]), values, preferred_element_type=jnp.float32
                )
                stats = stats_ref[rows]
                sums = sums * stats[:, 3:4]
                rest = sums - sums.astype(jnp.bfloat16).astype(jnp.float32)
                rest = jnp.where(lane < STATS, stats, rest)
                even = jnp.where(row < 4, sums, pltpu.roll(rest, 4, 0))
                odd = jnp.where(row < 4, pltpu.roll(sums, 4, 0), rest)
                out_ref[2 * turn] = even.astype(jnp.bfloat16)
                out_ref[2 * turn + 1] = odd.astype(jnp.bfloat16)
            return carry

        return step

    lax.fori_loop(0, KVH // 2 // UNROLL, value(v_ref, 0), 0)
    later.wait()
    lax.fori_loop(0, KVH // 2 // UNROLL, value(later_ref, KVH // 2), 0)


def merge_blocks(blocks_ref, own_ref, out_ref):
    blocks = blocks_ref[...].astype(jnp.float32)
    lane = lax.broadcasted_iota(jnp.int32, (4, HD), 1)
    sums = blocks[:, 0:4, :] + jnp.where(lane < STATS, 0.0, blocks[:, 4:8, :])
    mark = blocks[:, 4:8, 0:1]
    total = blocks[:, 4:8, 1:2] + blocks[:, 4:8, 2:3]
    new_score = own_ref[0:4, 0:1]
    top = jnp.maximum(jnp.max(mark, axis=0), new_score)
    factor = jnp.exp(mark - top[None])
    own = jnp.exp(new_score - top)
    denominator = jnp.sum(total * factor, axis=0) + own
    numerator = jnp.sum(sums * factor, axis=0) + own * own_ref[4:8]
    attention = (numerator / denominator).astype(jnp.bfloat16)
    out_ref[...] = jnp.broadcast_to(attention[None], out_ref.shape)


def project(attention_ref, w_ref, out_ref):
    blocks = attention_ref[...].astype(jnp.float32)
    rows = jnp.concatenate([blocks[GROUPS.index(k)] for k in PAIRS]).astype(jnp.bfloat16)
    out_ref[...] = lax.dot_general(
        rows, w_ref[...], (((1,), (1,)), ((), ())), preferred_element_type=jnp.float32
    ).astype(jnp.bfloat16)


def merged_attention(
    queries, key_cache, value_cache, new_key, new_value, page_table, counts, offsets, groups
):
    requests = queries.shape[0]
    peers = lax.axis_size(SEQ)
    vmem = pl.BlockSpec(memory_space=pltpu.VMEM)
    hbm = pl.BlockSpec(memory_space=pltpu.HBM)
    half = (*value_cache.shape[:2], value_cache.shape[2] // 2)
    small = pltpu.CompilerParams(vmem_limit_bytes=8 << 20)

    def near(x):
        return pltpu.with_memory_space_constraint(x, pltpu.VMEM)

    def far(x):
        return pltpu.with_memory_space_constraint(x, pltpu.HBM)

    spread, keys, values, rows, own = pl.pallas_call(
        fetch_pages,
        out_shape=(
            pltpu.VMEM((peers, *queries.shape), queries.dtype),
            pltpu.VMEM(key_cache.shape, key_cache.dtype),
            pltpu.VMEM(half, value_cache.dtype),
            pltpu.VMEM((3, 8, HD), jnp.int32),
            pltpu.VMEM((8, HD), jnp.float32),
        ),
        in_specs=[hbm] * 8,
        out_specs=(vmem,) * 5,
        scratch_shapes=[pltpu.SMEM((requests,), jnp.int32)] * 3
        + [pltpu.VMEM((requests, HD), jnp.bfloat16)] * 3
        + [pltpu.SemaphoreType.DMA((8,))],
        compiler_params=small,
    )(
        far(page_table[:, 0]), far(counts[:, 0]), far(offsets),
        far(queries), far(new_key), far(new_value), far(key_cache), far(value_cache),
    )
    all_queries = exchange(spread, SEQ, ORDER)
    blocks = pl.pallas_call(
        attend_pages,
        out_shape=pltpu.VMEM((HEADS, 8, HD), jnp.bfloat16),
        in_specs=[vmem, vmem, vmem, hbm, vmem],
        out_specs=vmem,
        scratch_shapes=[pltpu.VMEM(half, value_cache.dtype)]
        + [pltpu.VMEM((HEADS * requests, HD), jnp.float32)] * 3
        + [pltpu.SemaphoreType.DMA],
        compiler_params=small,
    )(
        near(all_queries.reshape(HEADS * requests, HD)),
        near(keys), near(values), far(value_cache), near(rows),
    )
    blocks = exchange(blocks, SEQ, ORDER)
    attention = pl.pallas_call(
        merge_blocks,
        out_shape=pltpu.VMEM((groups, requests, HD), jnp.bfloat16),
        in_specs=[vmem] * 2,
        out_specs=vmem,
        compiler_params=small,
    )(near(blocks), near(own))
    return attention


def on_device(
    queries, key_cache, value_cache, new_key, new_value, page_table, counts, offsets, w_out
):
    requests = queries.shape[0]
    peers = lax.axis_size(SEQ)
    groups = lax.axis_size(BATCH)
    attention = merged_attention(
        queries, key_cache, value_cache, new_key, new_value, page_table, counts, offsets, groups
    )
    attention = exchange(attention, BATCH, GROUPS)
    vmem = pl.BlockSpec(memory_space=pltpu.VMEM)
    partial = pl.pallas_call(
        project,
        out_shape=pltpu.VMEM((groups * requests, w_out.shape[1]), jnp.bfloat16),
        in_specs=[vmem] * 2,
        out_specs=vmem,
        compiler_params=pltpu.CompilerParams(vmem_limit_bytes=8 << 20),
    )(
        pltpu.with_memory_space_constraint(attention, pltpu.VMEM),
        pltpu.with_memory_space_constraint(w_out.T, pltpu.VMEM),
    )
    partial = partial.reshape(peers, -1, partial.shape[1])
    partial = exchange(partial, SEQ, ORDER)
    return jnp.sum(partial.astype(jnp.float32), axis=0).astype(jnp.bfloat16)


def solution(mesh):
    in_specs = (
        P(BATCH, SEQ),
        P(BATCH, SEQ, None),
        P(BATCH, SEQ, None),
        P(BATCH, None),
        P(BATCH, None),
        P(BATCH, SEQ),
        P(BATCH, SEQ),
        P(BATCH),
        P(SEQ, BATCH),
    )
    return jax.shard_map(
        on_device, mesh=mesh, in_specs=in_specs, out_specs=P(SEQ, BATCH), check_vma=False
    )
```
